32 devices in a mesh: chan: 4 (over z), pulse: 4 (over x, core), range: 2 (over y).
Axes of the slice: x: 2, y: 2, z: 4, core: 2. Of those that a mesh axis runs over, the one named last changes fastest.
Arguments:
- signal: bfloat16 [2, 64, 32, 8192], P(None, 'chan', 'pulse', 'range'), may hold values from -6 to 6
- steering: bfloat16 [2, 32, 64], replicated, may hold values from -0.5 to 0.5
- spectrum: float32 [2, 8192], replicated, may hold values from -6 to 6
Outputs:
- detection: float32 [32, 32, 8192], P('chan', 'pulse', 'range')
The draws below stay inside these ranges and needn't reach their ends.
All inputs are finite; a program needn't handle non-finite values.
Results may differ from the reference program's by a relative error of at most 0.0087.
Values may be sent and summed in bfloat16 or wider, within the bound.
No kernel may reach another device: no remote copies, remote signals or barrier semaphores. Data moves between devices by JAX's collectives and lax.ppermute only.
A program may use at most 64 MiB of HBM per device.

```python
import math
import jax
import jax.numpy as jnp
from jax import lax

CH = 64
BEAMS = 32
GUARD = 4
TRAIN = 16
PULSES = 32
RANGE = 8192


def block_levels(own_key, shape, pieces, low, top_value):
    loudness, own = 1.0, jax.random.fold_in(own_key, 6)
    for position, blocks in pieces:
        draws = jnp.exp(jax.random.uniform(jax.random.fold_in(own, position), (blocks,), jnp.float32, low / len(pieces), top_value / len(pieces)))
        loudness = loudness * jnp.repeat(draws, shape[position] // blocks).reshape([-1 if axis == position else 1 for axis in range(len(shape))])
    return loudness


def scatter_about(stream_key, extent, width, reach, split=(), held_as=jnp.bfloat16):
    entries = jax.random.normal(stream_key, extent, jnp.float32) * width
    if len(split) > 0:
        entries = block_levels(stream_key, extent, split, -0.22, 0.18) * entries
    return jnp.clip(entries, min=-reach, max=reach).astype(held_as)


def setup_inputs(seed: int = 0) -> dict:
    splits = jax.random.split(jax.random.key(seed), 4)
    return {
        "signal": scatter_about(splits[0], (2, CH, PULSES, RANGE), 1.0, 6.0, ((1, 4), (2, 4), (3, 2))),
        "steering": scatter_about(splits[1], (2, BEAMS, CH), (2 * CH) ** -0.5, 0.5),
        "spectrum": scatter_about(splits[2], (2, RANGE), 1.0, 6.0, (), jnp.float32),
    }


NOISE_FLOOR = 0.25

def doppler_tables(pulse_count):
    row_ids = lax.broadcasted_iota(jnp.int32, (pulse_count, pulse_count), 0)
    col_ids = lax.broadcasted_iota(jnp.int32, (pulse_count, pulse_count), 1)
    phase_angle = (row_ids * col_ids % pulse_count).astype(jnp.float32) * (2.0 * math.pi / pulse_count)
    norm_scale = 1.0 / math.sqrt(pulse_count)
    table_real = (jnp.cos(phase_angle) * norm_scale).astype(jnp.bfloat16)
    table_imag = (-jnp.sin(phase_angle) * norm_scale).astype(jnp.bfloat16)
    return (table_real, table_imag)

def reference(signal, steering, spectrum):
    w_real = steering[0]
    w_imag = steering[1]
    stacked = jnp.concatenate([jnp.concatenate([w_real, -w_imag], 1), jnp.concatenate([w_imag, w_real], 1)], 0)
    flat_signal = signal.reshape(2 * CH, PULSES * RANGE)
    beam_data = jnp.dot(stacked, flat_signal, preferred_element_type=jnp.float32).astype(jnp.bfloat16)
    beam_data = beam_data.reshape(2, BEAMS, PULSES, RANGE)
    response = lax.complex(spectrum[0], spectrum[1])
    dop_real, dop_imag = doppler_tables(PULSES)
    halo_width = GUARD + TRAIN

    def one_beam(beam_slab):
        line_field = lax.complex(beam_slab[0].astype(jnp.float32), beam_slab[1].astype(jnp.float32))
        compressed = jnp.fft.ifft(jnp.fft.fft(line_field, axis=-1) * response, axis=-1)
        comp_real = jnp.real(compressed).astype(jnp.bfloat16)
        comp_imag = jnp.imag(compressed).astype(jnp.bfloat16)
        mixed_real = jnp.dot(dop_real, comp_real, preferred_element_type=jnp.float32) - jnp.dot(dop_imag, comp_imag, preferred_element_type=jnp.float32)
        mixed_imag = jnp.dot(dop_real, comp_imag, preferred_element_type=jnp.float32) + jnp.dot(dop_imag, comp_real, preferred_element_type=jnp.float32)
        power_map = mixed_real * mixed_real + mixed_imag * mixed_imag
        padded = jnp.pad(power_map, ((0, 0), (halo_width, halo_width)))
        window_sum = jnp.zeros_like(power_map)
        for offset in range(1, TRAIN + 1):
            left_start = halo_width - GUARD - offset
            right_start = halo_width + GUARD + offset
            window_sum = window_sum + padded[:, left_start:left_start + RANGE] + padded[:, right_start:right_start + RANGE]
        noise_level = window_sum / (2.0 * TRAIN)
        return power_map / (noise_level + NOISE_FLOOR)
    return lax.map(one_beam, jnp.transpose(beam_data, (1, 0, 2, 3)))
```

```python
import functools
import math

import jax
import jax.numpy as jnp
import numpy as np
from jax import lax
from jax.experimental import pallas as pl
from jax.experimental.pallas import tpu as pltpu
from jax.sharding import PartitionSpec as P

GUARD = 4
TRAIN = 16
NOISE_FLOOR = 0.25
LANES = 128


def dft_pair(n):
    ids = np.arange(n)
    angle = 2.0 * np.pi * (np.outer(ids, ids) % n) / n
    return np.cos(angle), np.sin(angle)


def range_tables(length):
    rows = length // LANES
    cos1, sin1 = dft_pair(rows)
    cos2, sin2 = dft_pair(LANES)
    left_fwd = np.block([[cos1, sin1], [-sin1, cos1]])
    left_inv = np.block([[cos1, -sin1], [sin1, cos1]])
    right_fwd = np.block([[cos2, -sin2], [sin2, cos2]])
    right_inv = np.block([[cos2, sin2], [-sin2, cos2]])
    angle = 2.0 * np.pi * (np.outer(np.arange(rows), np.arange(LANES)) % length) / length
    twiddle = np.stack([np.cos(angle), -np.sin(angle)])
    mats = [jnp.asarray(m, jnp.bfloat16) for m in (left_fwd, left_inv, right_fwd, right_inv)]
    return mats + [jnp.asarray(twiddle, jnp.float32)]


def doppler_matrix(pulses):
    ids = np.arange(pulses)
    angle = 2.0 * np.pi * (np.outer(ids, ids) % pulses) / pulses
    scale = 1.0 / math.sqrt(pulses)
    real, imag = np.cos(angle) * scale, -np.sin(angle) * scale
    return jnp.asarray(np.block([[real, -imag], [imag, real]]), jnp.bfloat16)


def filter_kernel(
    beams, rows, x_ref, w_ref, lf_ref, li_ref, rf_ref, ri_ref, tw_ref, h_ref, out_ref, s_ref, a_ref
):
    blocks = x_ref.shape[1]
    gates = x_ref.shape[4]
    depth = w_ref.shape[1]
    per_block = gates // LANES
    wide = 8
    for block in range(blocks):
        for step in range(per_block // wide):
            lanes = pl.ds(step * wide * LANES, wide * LANES)
            x = x_ref[:, block, :, :, lanes].reshape(depth, wide * LANES)
            y = jnp.dot(w_ref[...], x, preferred_element_type=jnp.float32)
            for i in range(wide):
                n1 = block * per_block + step * wide + i
                s_ref[pl.ds(n1, 2 * beams, stride=rows), :] = y[:, i * LANES : (i + 1) * LANES]
    group = 4
    scale = 1.0 / (rows * LANES)
    tw_re, tw_im = tw_ref[0], tw_ref[1]
    h_re, h_im = h_ref[0], h_ref[1]

    def spun(z, c_re, c_im):
        re, im = z[:, :LANES], z[:, LANES:]
        return jnp.concatenate([re * c_re - im * c_im, re * c_im + im * c_re], 1)

    def body(g, carry):
        for i in range(group):
            b = g * group + i
            re = s_ref[pl.ds(pl.multiple_of(b * rows, rows), rows), :]
            im = s_ref[pl.ds(pl.multiple_of((b + beams) * rows, rows), rows), :]
            z = jnp.concatenate([re, im], 0).astype(jnp.bfloat16)
            a = jnp.dot(lf_ref[...], z, preferred_element_type=jnp.float32)
            z = spun(jnp.concatenate([a[:rows], a[rows:]], 1), tw_re, tw_im)
            a_ref[pl.ds(i * rows, rows), :] = z.astype(jnp.bfloat16)
        c = jnp.dot(a_ref[...], rf_ref[...], preferred_element_type=jnp.float32)
        d = jnp.concatenate(
            [spun(c[i * rows : (i + 1) * rows], h_re, h_im) for i in range(group)], 0
        ).astype(jnp.bfloat16)
        e = jnp.dot(d, ri_ref[...], preferred_element_type=jnp.float32)
        for i in range(group):
            b = g * group + i
            z = spun(e[i * rows : (i + 1) * rows], tw_re * scale, -tw_im * scale)
            z = jnp.concatenate([z[:, :LANES], z[:, LANES:]], 0).astype(jnp.bfloat16)
            o = jnp.dot(li_ref[...], z, preferred_element_type=jnp.float32)
            out_ref[b] = o.astype(jnp.bfloat16)
        return carry

    lax.fori_loop(0, beams // group, body, 0)


def detect_kernel(pulses, rows, z_ref, d_ref, out_ref, s_ref, p_ref):
    parts, halves, bins, gates = out_ref.shape
    length = rows * LANES
    for p in range(pulses):
        s_ref[pl.ds(p * 2 * rows, 2 * rows), :] = z_ref[p].astype(jnp.float32)
    p_ref[:, pl.ds(0, LANES)] = jnp.zeros((pulses, LANES), jnp.float32)
    p_ref[:, pl.ds(LANES + length, LANES)] = jnp.zeros((pulses, LANES), jnp.float32)
    wide = 8

    def body(step, carry):
        cols = []
        for i in range(wide):
            j = step * wide + i
            re = s_ref[pl.ds(j, pulses, stride=2 * rows), :]
            im = s_ref[pl.ds(j + rows, pulses, stride=2 * rows), :]
            cols.append(jnp.concatenate([re, im], 0).astype(jnp.bfloat16))
        m = jnp.dot(d_ref[...], jnp.concatenate(cols, 1), preferred_element_type=jnp.float32)
        re, im = m[:pulses], m[pulses:]
        at = pl.multiple_of(LANES + step * wide * LANES, LANES)
        p_ref[:, pl.ds(at, wide * LANES)] = re * re + im * im
        return carry

    lax.fori_loop(0, rows // wide, body, 0)
    span = length + 2 * LANES
    for q in range(parts):
        power = p_ref[pl.ds(q * bins, bins), :]
        total, width = power, 1
        while width < TRAIN:
            total = total + pltpu.roll(total, span - width, 1)
            width *= 2
        noise = pltpu.roll(total, GUARD + TRAIN, 1) + pltpu.roll(total, span - GUARD - 1, 1)
        found = power / (noise * (1.0 / (2 * TRAIN)) + NOISE_FLOOR)
        for s in range(halves):
            out_ref[q, s] = found[:, LANES + s * gates : LANES + (s + 1) * gates].astype(
                jnp.bfloat16
            )


def stack_weights(w_real, w_imag):
    return jnp.concatenate(
        [jnp.concatenate([w_real, -w_imag], 1), jnp.concatenate([w_imag, w_real], 1)], 0
    )


def vmem_call(kernel, out_shape, scratch, flops, *args):
    return pl.pallas_call(
        kernel,
        out_shape=out_shape,
        in_specs=[pl.BlockSpec(memory_space=pltpu.VMEM)] * len(args),
        out_specs=pl.BlockSpec(memory_space=pltpu.VMEM),
        scratch_shapes=scratch,
        cost_estimate=pl.CostEstimate(flops=flops, bytes_accessed=0, transcendentals=0),
        compiler_params=pltpu.CompilerParams(vmem_limit_bytes=48 * 1024 * 1024),
    )(*args)


def lines(signal, steering, spectrum):
    chans, pulses_n, halves = (lax.axis_size(a) for a in ("chan", "pulse", "range"))
    beams, channels = steering.shape[1:]
    pulse_local, gates = signal.shape[2:]
    pulses, length = pulse_local * pulses_n, gates * halves
    rows = length // LANES
    chan_local = channels // chans
    parts = pulses_n * halves
    everyone = ("pulse", "chan", "range")

    moved = jnp.transpose(signal, (2, 0, 1, 3))
    moved = lax.all_to_all(moved, ("chan", "range"), 0, 0, tiled=True)
    moved = moved.reshape(chans, halves, 2, chan_local, gates)

    weights = steering.reshape(2, chans, pulses_n, halves, channels)
    weights = jnp.transpose(weights, (0, 2, 1, 3, 4)).reshape(2, beams, channels)
    weights = stack_weights(weights[0], weights[1]).reshape(2 * beams, 2, chans, chan_local)
    weights = jnp.transpose(weights, (0, 2, 1, 3)).reshape(2 * beams, 2 * channels)
    response = jnp.transpose(spectrum.reshape(2, LANES, rows), (0, 2, 1))
    lf, li, rf, ri, twiddle = range_tables(length)
    compressed = vmem_call(
        functools.partial(filter_kernel, beams, rows),
        jax.ShapeDtypeStruct((beams, 2 * rows, LANES), jnp.bfloat16),
        [
            pltpu.VMEM((2 * beams * rows, LANES), jnp.float32),
            pltpu.VMEM((4 * rows, 2 * LANES), jnp.bfloat16),
        ],
        2_000_000_000,
        moved, weights, lf, li, rf, ri, twiddle, response,
    )
    columns = lax.all_to_all(compressed, everyone, 0, 0, tiled=True)
    bins = pulses // pulses_n
    found = vmem_call(
        functools.partial(detect_kernel, pulses, rows),
        jax.ShapeDtypeStruct((pulses_n, halves, bins, gates), jnp.bfloat16),
        [
            pltpu.VMEM((pulses * 2 * rows, LANES), jnp.float32),
            pltpu.VMEM((pulses, length + 2 * LANES), jnp.float32),
        ],
        2_000_000_000,
        columns, doppler_matrix(pulses),
    )
    found = found.reshape(parts, bins, gates)
    found = lax.all_to_all(found, ("pulse", "range"), 0, 0, tiled=True)
    return found.astype(jnp.float32)


PRECISE = lax.Precision.HIGHEST


def padded_2(x, sides, width):
    for axis, dim in sides:
        peers, length = (lax.axis_size(axis), x.shape[dim])
        up = [(i, (i + 1) % peers) for i in range(peers - 1)]
        down = [(j, i) for i, j in up]
        last = lax.slice_in_dim(x, length - width, length, axis=dim)
        initial = lax.slice_in_dim(x, 0, width, axis=dim)
        before = lax.ppermute(last, axis, up)
        after = lax.ppermute(initial, axis, down)
        x = jnp.concatenate([before, x, after], axis=dim)
    return x


def doppler_tables(pulse_count):
    row_ids = lax.broadcasted_iota(jnp.int32, (pulse_count, pulse_count), 0)
    col_ids = lax.broadcasted_iota(jnp.int32, (pulse_count, pulse_count), 1)
    phase_angle = (row_ids * col_ids % pulse_count).astype(jnp.float32) * (
        2.0 * math.pi / pulse_count
    )
    norm_scale = 1.0 / math.sqrt(pulse_count)
    table_real = (jnp.cos(phase_angle) * norm_scale).astype(jnp.bfloat16)
    table_imag = (-jnp.sin(phase_angle) * norm_scale).astype(jnp.bfloat16)
    return (table_real, table_imag)


def phase_table(row_count, col_count, period_len, direction):
    row_ids = lax.broadcasted_iota(jnp.int32, (row_count, col_count), 0)
    col_ids = lax.broadcasted_iota(jnp.int32, (row_count, col_count), 1)
    phase_angle = (row_ids * col_ids % period_len).astype(jnp.float32) * (
        2.0 * math.pi / period_len
    )
    return (jnp.cos(phase_angle), direction * jnp.sin(phase_angle))


def rotate_by(field_pair, table_pair):
    return (
        field_pair[0] * table_pair[0] - field_pair[1] * table_pair[1],
        field_pair[0] * table_pair[1] + field_pair[1] * table_pair[0],
    )


def mix_blocks(table_pair, field_pair):

    def contract(table_part, field_part):
        return jnp.einsum("km,bpmn->bpkn", table_part, field_part, precision=PRECISE)

    return (
        contract(table_pair[0], field_pair[0]) - contract(table_pair[1], field_pair[1]),
        contract(table_pair[0], field_pair[1]) + contract(table_pair[1], field_pair[0]),
    )


def mix_lanes(field_pair, table_pair):

    def contract(field_part, table_part):
        return jnp.einsum("bpkm,mn->bpkn", field_part, table_part, precision=PRECISE)

    return (
        contract(field_pair[0], table_pair[0]) - contract(field_pair[1], table_pair[1]),
        contract(field_pair[0], table_pair[1]) + contract(field_pair[1], table_pair[0]),
    )


def local_transform(field_pair, direction):
    size_all = field_pair[0].shape[-1]
    blocks = size_all // 128
    leading = field_pair[0].shape[:-1]
    shaped = tuple((member.reshape(leading + (blocks, 128)) for member in field_pair))
    outer_table = phase_table(blocks, blocks, blocks, direction)
    twiddle = phase_table(blocks, 128, size_all, direction)
    inner_table = phase_table(128, 128, 128, direction)
    if direction < 0:
        shaped = mix_blocks(outer_table, shaped)
        shaped = rotate_by(shaped, twiddle)
        shaped = mix_lanes(shaped, inner_table)
    else:
        shaped = mix_lanes(shaped, inner_table)
        shaped = rotate_by(shaped, twiddle)
        shaped = mix_blocks(outer_table, shaped)
    return tuple((member.reshape(leading + (size_all,)) for member in shaped))


def blocks(signal, steering, spectrum):
    beam_count = steering.shape[1]
    chan_count = steering.shape[2]
    pulse_local = signal.shape[2]
    gate_count = signal.shape[3]
    stacked = stack_weights(steering[0], steering[1])
    samples = lax.all_to_all(signal, "chan", split_axis=2, concat_axis=1, tiled=True)
    pulses_here = samples.shape[2]
    gates_here = samples.shape[3]
    flat_samples = samples.reshape(2 * chan_count, pulses_here * gates_here)
    formed = jnp.dot(stacked, flat_samples, preferred_element_type=jnp.float32)
    formed = formed.astype(jnp.bfloat16).reshape(2, beam_count, pulses_here, gates_here)
    beam_data = lax.all_to_all(formed, "chan", split_axis=1, concat_axis=2, tiled=True)
    beam_local = beam_data.shape[1]
    range_count = lax.axis_size("range")
    range_index = lax.axis_index("range")
    full_length = gate_count * range_count
    inverse_scale = 1.0 / full_length
    shard_piece = lax.all_gather(beam_data, "range", axis=3, tiled=True)
    shard_count = shard_piece.shape[3] // gate_count
    members = shard_piece.astype(jnp.float32).reshape(
        2, beam_local, pulse_local, shard_count, gate_count
    )
    source = jnp.arange(shard_count, dtype=jnp.int32)
    phase_angle = (source * range_index % range_count).astype(jnp.float32) * (
        2.0 * math.pi / range_count
    )
    cos_part = jnp.cos(phase_angle)[:, None]
    sin_part = -jnp.sin(phase_angle)[:, None]
    sum_real = jnp.sum(members[0] * cos_part - members[1] * sin_part, axis=2)
    sum_imag = jnp.sum(members[0] * sin_part + members[1] * cos_part, axis=2)
    folded = (sum_real, sum_imag)
    gate_ids = lax.broadcasted_iota(jnp.int32, (gate_count,), 0)
    global_angle = (gate_ids * range_index % full_length).astype(jnp.float32) * (
        2.0 * math.pi / full_length
    )
    folded = rotate_by(folded, (jnp.cos(global_angle), -jnp.sin(global_angle)))
    spectrum_local = local_transform(folded, -1.0)
    response = spectrum.reshape(2, gate_count, range_count)
    response = lax.dynamic_index_in_dim(response, range_index, axis=2, keepdims=False)
    response = jnp.transpose(response.reshape(2, 128, gate_count // 128), (0, 2, 1)).reshape(
        2, gate_count
    )
    filtered = rotate_by(spectrum_local, (response[0], response[1]))
    restored = local_transform(filtered, 1.0)
    restored = rotate_by(restored, (jnp.cos(global_angle), jnp.sin(global_angle)))
    shard_piece = (
        lax.all_gather(restored[0], "range", axis=2, tiled=True),
        lax.all_gather(restored[1], "range", axis=2, tiled=True),
    )
    shard_count = shard_piece[0].shape[2] // gate_count
    rows_real = shard_piece[0].reshape(beam_local, pulse_local, shard_count, gate_count)
    rows_imag = shard_piece[1].reshape(beam_local, pulse_local, shard_count, gate_count)
    source = jnp.arange(shard_count, dtype=jnp.int32)
    phase_angle = (source * range_index % range_count).astype(jnp.float32) * (
        2.0 * math.pi / range_count
    )
    cos_part = jnp.cos(phase_angle)[:, None]
    sin_part = jnp.sin(phase_angle)[:, None]
    sum_real = jnp.sum(rows_real * cos_part - rows_imag * sin_part, axis=2)
    sum_imag = jnp.sum(rows_real * sin_part + rows_imag * cos_part, axis=2)
    compressed = jnp.stack([sum_real * inverse_scale, sum_imag * inverse_scale]).astype(
        jnp.bfloat16
    )
    pulse_total = pulse_local * lax.axis_size("pulse")
    dop_real, dop_imag = doppler_tables(pulse_total)
    columns = lax.all_to_all(compressed, "pulse", split_axis=3, concat_axis=2, tiled=True)

    def product(table_part, values):
        return jnp.einsum("fp,bpr->bfr", table_part, values, preferred_element_type=jnp.float32)

    mixed_real = product(dop_real, columns[0]) - product(dop_imag, columns[1])
    mixed_imag = product(dop_real, columns[1]) + product(dop_imag, columns[0])
    power_part = lax.all_to_all(
        mixed_real * mixed_real + mixed_imag * mixed_imag,
        "pulse",
        split_axis=1,
        concat_axis=2,
        tiled=True,
    )
    halo_width = GUARD + TRAIN
    padded = padded_2(power_part, (("range", 2),), halo_width)
    window_sum = jnp.zeros_like(power_part)
    for offset in range(1, TRAIN + 1):
        left_start = halo_width - GUARD - offset
        right_start = halo_width + GUARD + offset
        window_sum = (
            window_sum
            + padded[:, :, left_start : left_start + gate_count]
            + padded[:, :, right_start : right_start + gate_count]
        )
    noise_level = window_sum / (2.0 * TRAIN)
    return power_part / (noise_level + NOISE_FLOOR)


def solution(mesh):
    in_specs = (P(None, "chan", "pulse", "range"), P(), P())
    out_specs = P("chan", "pulse", "range")

    def shards(signal, steering, spectrum):
        sizes = {a: lax.axis_size(a) for a in mesh.axis_names}
        beam_local = steering.shape[1] // sizes["chan"]
        if beam_local == sizes["pulse"] * sizes["range"] and signal.shape[2] == (
            sizes["chan"] * sizes["range"]
        ):
            return lines(signal, steering, spectrum)
        return blocks(signal, steering, spectrum)

    return jax.shard_map(shards, mesh=mesh, in_specs=in_specs, out_specs=out_specs, check_vma=False)
```

```python
import functools
import math

import jax
import jax.numpy as jnp
import numpy as np
from jax import lax
from jax.experimental import pallas as pl
from jax.experimental.pallas import tpu as pltpu
from jax.sharding import PartitionSpec as P

GUARD = 4
TRAIN = 16
NOISE_FLOOR = 0.25
LANES = 128


def dft_pair(n):
    ids = np.arange(n)
    angle = 2.0 * np.pi * (np.outer(ids, ids) % n) / n
    return np.cos(angle), np.sin(angle)


def range_tables(length):
    rows = length // LANES
    cos1, sin1 = dft_pair(rows)
    cos2, sin2 = dft_pair(LANES)
    left_fwd = np.block([[cos1, sin1], [-sin1, cos1]])
    left_inv = np.block([[cos1, -sin1], [sin1, cos1]])
    right_fwd = np.block([[cos2, -sin2], [sin2, cos2]])
    right_inv = np.block([[cos2, sin2], [-sin2, cos2]])
    angle = 2.0 * np.pi * (np.outer(np.arange(rows), np.arange(LANES)) % length) / length
    twiddle = np.stack([np.cos(angle), -np.sin(angle)])
    mats = [jnp.asarray(m, jnp.bfloat16) for m in (left_fwd, left_inv, right_fwd, right_inv)]
    return mats + [jnp.asarray(twiddle, jnp.float32)]


def doppler_matrix(pulses):
    ids = np.arange(pulses)
    angle = 2.0 * np.pi * (np.outer(ids, ids) % pulses) / pulses
    scale = 1.0 / math.sqrt(pulses)
    real, imag = np.cos(angle) * scale, -np.sin(angle) * scale
    return jnp.asarray(np.block([[real, -imag], [imag, real]]), jnp.bfloat16)


def partial_kernel(x0_ref, x1_ref, x2_ref, x3_ref, w_ref, out_ref):
    for side, pair in enumerate(((x0_ref, x2_ref), (x1_ref, x3_ref))):
        out_ref[side] = formed(w_ref, pair, slice(None)).astype(jnp.bfloat16)


def formed(w_ref, pair, lanes):
    x = jnp.concatenate([r[:, :, lanes].reshape(-1, r[:, :, lanes].shape[-1]) for r in pair], 0)
    return jnp.dot(w_ref[...], x, preferred_element_type=jnp.float32)


def filter_kernel(
    beams, rows, at_ref, x0_ref, x1_ref, x2_ref, x3_ref, w_ref, more_ref, after_ref,
    lf_ref, li_ref, rf_ref, ri_ref, tw_ref, h_ref, out_ref, s_ref, a_ref
):
    gates = x0_ref.shape[2]
    per_block = gates // LANES
    wide = 8
    for side, pair in enumerate(((x0_ref, x2_ref), (x1_ref, x3_ref))):
        base = at_ref[side] * per_block
        for step in range(per_block // wide):
            lanes = pl.ds(step * wide * LANES, wide * LANES)
            y = formed(w_ref, pair, lanes) + more_ref[side, :, lanes].astype(jnp.float32)
            for i in range(wide):
                n1 = base + (step * wide + i)
                s_ref[pl.ds(n1, 2 * beams, stride=rows), :] = y[:, i * LANES : (i + 1) * LANES]
    group = 4
    scale = 1.0 / (rows * LANES)
    tw_re, tw_im = tw_ref[0], tw_ref[1]
    h_re, h_im = h_ref[0], h_ref[1]

    def spun(z, c_re, c_im):
        re, im = z[:, :LANES], z[:, LANES:]
        return jnp.concatenate([re * c_re - im * c_im, re * c_im + im * c_re], 1)

    def body(g, carry):
        for i in range(group):
            b = g * group + i
            re = s_ref[pl.ds(pl.multiple_of(b * rows, rows), rows), :]
            im = s_ref[pl.ds(pl.multiple_of((b + beams) * rows, rows), rows), :]
            z = jnp.concatenate([re, im], 0).astype(jnp.bfloat16)
            a = jnp.dot(lf_ref[...], z, preferred_element_type=jnp.float32)
            z = spun(jnp.concatenate([a[:rows], a[rows:]], 1), tw_re, tw_im)
            a_ref[pl.ds(i * rows, rows), :] = z.astype(jnp.bfloat16)
        c = jnp.dot(a_ref[...], rf_ref[...], preferred_element_type=jnp.float32)
        d = jnp.concatenate(
            [spun(c[i * rows : (i + 1) * rows], h_re, h_im) for i in range(group)], 0
        ).astype(jnp.bfloat16)
        e = jnp.dot(d, ri_ref[...], preferred_element_type=jnp.float32)
        for i in range(group):
            b = g * group + i
            z = spun(e[i * rows : (i + 1) * rows], tw_re * scale, -tw_im * scale)
            z = jnp.concatenate([z[:, :LANES], z[:, LANES:]], 0).astype(jnp.bfloat16)
            o = jnp.dot(li_ref[...], z, preferred_element_type=jnp.float32)
            out_ref[b] = o.astype(jnp.bfloat16)
        return carry

    lax.fori_loop(0, beams // group, body, 0)


def detect_kernel(pulses, rows, group, z0_ref, z1_ref, d_ref, out_ref, s_ref, p_ref):
    parts, halves, bins, gates = out_ref.shape
    length = rows * LANES
    for part, z_ref in enumerate((z0_ref, z1_ref)):
        for i in range(pulses // 2):
            p = i // group * 2 * group + part * group + i % group
            s_ref[pl.ds(p * 2 * rows, 2 * rows), :] = z_ref[i].astype(jnp.float32)
    p_ref[:, pl.ds(0, LANES)] = jnp.zeros((pulses, LANES), jnp.float32)
    p_ref[:, pl.ds(LANES + length, LANES)] = jnp.zeros((pulses, LANES), jnp.float32)
    wide = 8

    def body(step, carry):
        cols = []
        for i in range(wide):
            j = step * wide + i
            re = s_ref[pl.ds(j, pulses, stride=2 * rows), :]
            im = s_ref[pl.ds(j + rows, pulses, stride=2 * rows), :]
            cols.append(jnp.concatenate([re, im], 0).astype(jnp.bfloat16))
        m = jnp.dot(d_ref[...], jnp.concatenate(cols, 1), preferred_element_type=jnp.float32)
        re, im = m[:pulses], m[pulses:]
        at = pl.multiple_of(LANES + step * wide * LANES, LANES)
        p_ref[:, pl.ds(at, wide * LANES)] = re * re + im * im
        return carry

    lax.fori_loop(0, rows // wide, body, 0)
    span = length + 2 * LANES
    for q in range(parts):
        power = p_ref[pl.ds(q * bins, bins), :]
        total, width = power, 1
        while width < TRAIN:
            total = total + pltpu.roll(total, span - width, 1)
            width *= 2
        noise = pltpu.roll(total, GUARD + TRAIN, 1) + pltpu.roll(total, span - GUARD - 1, 1)
        found = power / (noise * (1.0 / (2 * TRAIN)) + NOISE_FLOOR)
        for s in range(halves):
            out_ref[q, s] = found[:, LANES + s * gates : LANES + (s + 1) * gates].astype(
                jnp.bfloat16
            )


def stack_weights(w_real, w_imag):
    return jnp.concatenate(
        [jnp.concatenate([w_real, -w_imag], 1), jnp.concatenate([w_imag, w_real], 1)], 0
    )


def vmem_call(kernel, out_shape, scratch, flops, *args, after=None):
    return pl.pallas_call(
        kernel,
        out_shape=out_shape,
        in_specs=[
            pl.BlockSpec(
                memory_space=pltpu.SMEM
                if a.dtype == jnp.int32
                else pl.ANY
                if a is after
                else pltpu.VMEM
            )
            for a in args
        ],
        out_specs=pl.BlockSpec(memory_space=pltpu.VMEM),
        scratch_shapes=scratch,
        cost_estimate=pl.CostEstimate(flops=flops, bytes_accessed=0, transcendentals=0),
        compiler_params=pltpu.CompilerParams(vmem_limit_bytes=48 * 1024 * 1024),
    )(*args)


def swapped(x, axes, flip):
    peers = lax.axis_size(axes)
    return lax.ppermute(x, axes, [(i, i ^ flip) for i in range(peers)])


def lines(signal, steering, spectrum):
    his, los, pulses_n, halves = (lax.axis_size(a) for a in ("hi", "lo", "pulse", "range"))
    beams, channels = steering.shape[1:]
    pulse_local, gates = signal.shape[2:]
    pulses, length = pulse_local * pulses_n, gates * halves
    rows = length // LANES
    chan_local = signal.shape[1]
    parts = pulses_n * halves
    near, group = ("lo", "range"), los * halves
    hi, lo, side = (lax.axis_index(a) for a in ("hi", "lo", "range"))
    me = lo * halves + side

    moved = jnp.transpose(signal, (2, 0, 1, 3))

    def block(part, flip):
        return lax.dynamic_index_in_dim(moved, part * group + (me ^ flip), 0, keepdims=False)

    pieces = [
        [block(part, 0)] + [swapped(block(part, flip), near, flip) for flip in range(1, group)]
        for part in range(2)
    ]

    half = beams // his
    weights = steering.reshape(2, his, los, pulses_n, halves, channels)
    weights = jnp.transpose(weights, (0, 1, 3, 2, 4, 5)).reshape(2, beams, channels)
    weights = stack_weights(weights[0], weights[1])
    weights = weights.reshape(2, his, half, 2, his, los, chan_local)
    weights = jnp.transpose(weights, (1, 4, 0, 2, 5, 3, 6))
    weights = lax.dynamic_index_in_dim(weights, hi, 1, keepdims=False)
    weights = jnp.where(lo == 0, weights, weights[:, :, :, ::-1])
    weights = weights.reshape(his, 2 * half, los * 2 * chan_local)
    w_own = lax.dynamic_index_in_dim(weights, hi, 0, keepdims=False)
    w_other = lax.dynamic_index_in_dim(weights, 1 - hi, 0, keepdims=False)
    response = jnp.transpose(spectrum.reshape(2, LANES, rows), (0, 2, 1))
    lf, li, rf, ri, twiddle = range_tables(length)
    at = jnp.stack([side, 1 - side]).astype(jnp.int32)

    sent = [
        vmem_call(
            partial_kernel,
            jax.ShapeDtypeStruct((halves, 2 * half, gates), jnp.bfloat16),
            [], 40_000_000, *piece, w_other,
        )
        for piece in pieces
    ]
    more = [swapped(x, "hi", 1) for x in sent]
    columns = []
    for piece, extra in zip(pieces, more):
        compressed = vmem_call(
            functools.partial(filter_kernel, half, rows),
            jax.ShapeDtypeStruct((half, 2 * rows, LANES), jnp.bfloat16),
            [
                pltpu.VMEM((2 * half * rows, LANES), jnp.float32),
                pltpu.VMEM((4 * rows, 2 * LANES), jnp.bfloat16),
            ],
            100_000_000,
            at, *piece, w_own, extra, sent[-1], lf, li, rf, ri, twiddle, response,
            after=sent[-1],
        )
        columns.append(lax.all_to_all(compressed, ("pulse", "lo", "range"), 0, 0, tiled=True))
    bins = pulses // pulses_n
    found = vmem_call(
        functools.partial(detect_kernel, pulses, rows, group),
        jax.ShapeDtypeStruct((pulses_n, halves, bins, gates), jnp.bfloat16),
        [
            pltpu.VMEM((pulses * 2 * rows, LANES), jnp.float32),
            pltpu.VMEM((pulses, length + 2 * LANES), jnp.float32),
        ],
        100_000_000,
        *columns, doppler_matrix(pulses),
    )
    found = found.reshape(parts, bins, gates)
    found = lax.all_to_all(found, ("pulse", "range"), 0, 0, tiled=True)
    return found.astype(jnp.float32)


PRECISE = lax.Precision.HIGHEST


def padded_2(x, sides, width):
    for axis, dim in sides:
        peers, length = (lax.axis_size(axis), x.shape[dim])
        up = [(i, (i + 1) % peers) for i in range(peers - 1)]
        down = [(j, i) for i, j in up]
        last = lax.slice_in_dim(x, length - width, length, axis=dim)
        initial = lax.slice_in_dim(x, 0, width, axis=dim)
        before = lax.ppermute(last, axis, up)
        after = lax.ppermute(initial, axis, down)
        x = jnp.concatenate([before, x, after], axis=dim)
    return x


def doppler_tables(pulse_count):
    row_ids = lax.broadcasted_iota(jnp.int32, (pulse_count, pulse_count), 0)
    col_ids = lax.broadcasted_iota(jnp.int32, (pulse_count, pulse_count), 1)
    phase_angle = (row_ids * col_ids % pulse_count).astype(jnp.float32) * (
        2.0 * math.pi / pulse_count
    )
    norm_scale = 1.0 / math.sqrt(pulse_count)
    table_real = (jnp.cos(phase_angle) * norm_scale).astype(jnp.bfloat16)
    table_imag = (-jnp.sin(phase_angle) * norm_scale).astype(jnp.bfloat16)
    return (table_real, table_imag)


def phase_table(row_count, col_count, period_len, direction):
    row_ids = lax.broadcasted_iota(jnp.int32, (row_count, col_count), 0)
    col_ids = lax.broadcasted_iota(jnp.int32, (row_count, col_count), 1)
    phase_angle = (row_ids * col_ids % period_len).astype(jnp.float32) * (
        2.0 * math.pi / period_len
    )
    return (jnp.cos(phase_angle), direction * jnp.sin(phase_angle))


def rotate_by(field_pair, table_pair):
    return (
        field_pair[0] * table_pair[0] - field_pair[1] * table_pair[1],
        field_pair[0] * table_pair[1] + field_pair[1] * table_pair[0],
    )


def mix_blocks(table_pair, field_pair):

    def contract(table_part, field_part):
        return jnp.einsum("km,bpmn->bpkn", table_part, field_part, precision=PRECISE)

    return (
        contract(table_pair[0], field_pair[0]) - contract(table_pair[1], field_pair[1]),
        contract(table_pair[0], field_pair[1]) + contract(table_pair[1], field_pair[0]),
    )


def mix_lanes(field_pair, table_pair):

    def contract(field_part, table_part):
        return jnp.einsum("bpkm,mn->bpkn", field_part, table_part, precision=PRECISE)

    return (
        contract(field_pair[0], table_pair[0]) - contract(field_pair[1], table_pair[1]),
        contract(field_pair[0], table_pair[1]) + contract(field_pair[1], table_pair[0]),
    )


def local_transform(field_pair, direction):
    size_all = field_pair[0].shape[-1]
    blocks = size_all // 128
    leading = field_pair[0].shape[:-1]
    shaped = tuple((member.reshape(leading + (blocks, 128)) for member in field_pair))
    outer_table = phase_table(blocks, blocks, blocks, direction)
    twiddle = phase_table(blocks, 128, size_all, direction)
    inner_table = phase_table(128, 128, 128, direction)
    if direction < 0:
        shaped = mix_blocks(outer_table, shaped)
        shaped = rotate_by(shaped, twiddle)
        shaped = mix_lanes(shaped, inner_table)
    else:
        shaped = mix_lanes(shaped, inner_table)
        shaped = rotate_by(shaped, twiddle)
        shaped = mix_blocks(outer_table, shaped)
    return tuple((member.reshape(leading + (size_all,)) for member in shaped))


def blocks(signal, steering, spectrum):
    beam_count = steering.shape[1]
    chan_count = steering.shape[2]
    pulse_local = signal.shape[2]
    gate_count = signal.shape[3]
    stacked = stack_weights(steering[0], steering[1])
    samples = lax.all_to_all(signal, "chan", split_axis=2, concat_axis=1, tiled=True)
    pulses_here = samples.shape[2]
    gates_here = samples.shape[3]
    flat_samples = samples.reshape(2 * chan_count, pulses_here * gates_here)
    formed = jnp.dot(stacked, flat_samples, preferred_element_type=jnp.float32)
    formed = formed.astype(jnp.bfloat16).reshape(2, beam_count, pulses_here, gates_here)
    beam_data = lax.all_to_all(formed, "chan", split_axis=1, concat_axis=2, tiled=True)
    beam_local = beam_data.shape[1]
    range_count = lax.axis_size("range")
    range_index = lax.axis_index("range")
    full_length = gate_count * range_count
    inverse_scale = 1.0 / full_length
    shard_piece = lax.all_gather(beam_data, "range", axis=3, tiled=True)
    shard_count = shard_piece.shape[3] // gate_count
    members = shard_piece.astype(jnp.float32).reshape(
        2, beam_local, pulse_local, shard_count, gate_count
    )
    source = jnp.arange(shard_count, dtype=jnp.int32)
    phase_angle = (source * range_index % range_count).astype(jnp.float32) * (
        2.0 * math.pi / range_count
    )
    cos_part = jnp.cos(phase_angle)[:, None]
    sin_part = -jnp.sin(phase_angle)[:, None]
    sum_real = jnp.sum(members[0] * cos_part - members[1] * sin_part, axis=2)
    sum_imag = jnp.sum(members[0] * sin_part + members[1] * cos_part, axis=2)
    folded = (sum_real, sum_imag)
    gate_ids = lax.broadcasted_iota(jnp.int32, (gate_count,), 0)
    global_angle = (gate_ids * range_index % full_length).astype(jnp.float32) * (
        2.0 * math.pi / full_length
    )
    folded = rotate_by(folded, (jnp.cos(global_angle), -jnp.sin(global_angle)))
    spectrum_local = local_transform(folded, -1.0)
    response = spectrum.reshape(2, gate_count, range_count)
    response = lax.dynamic_index_in_dim(response, range_index, axis=2, keepdims=False)
    response = jnp.transpose(response.reshape(2, 128, gate_count // 128), (0, 2, 1)).reshape(
        2, gate_count
    )
    filtered = rotate_by(spectrum_local, (response[0], response[1]))
    restored = local_transform(filtered, 1.0)
    restored = rotate_by(restored, (jnp.cos(global_angle), jnp.sin(global_angle)))
    shard_piece = (
        lax.all_gather(restored[0], "range", axis=2, tiled=True),
        lax.all_gather(restored[1], "range", axis=2, tiled=True),
    )
    shard_count = shard_piece[0].shape[2] // gate_count
    rows_real = shard_piece[0].reshape(beam_local, pulse_local, shard_count, gate_count)
    rows_imag = shard_piece[1].reshape(beam_local, pulse_local, shard_count, gate_count)
    source = jnp.arange(shard_count, dtype=jnp.int32)
    phase_angle = (source * range_index % range_count).astype(jnp.float32) * (
        2.0 * math.pi / range_count
    )
    cos_part = jnp.cos(phase_angle)[:, None]
    sin_part = jnp.sin(phase_angle)[:, None]
    sum_real = jnp.sum(rows_real * cos_part - rows_imag * sin_part, axis=2)
    sum_imag = jnp.sum(rows_real * sin_part + rows_imag * cos_part, axis=2)
    compressed = jnp.stack([sum_real * inverse_scale, sum_imag * inverse_scale]).astype(
        jnp.bfloat16
    )
    pulse_total = pulse_local * lax.axis_size("pulse")
    dop_real, dop_imag = doppler_tables(pulse_total)
    columns = lax.all_to_all(compressed, "pulse", split_axis=3, concat_axis=2, tiled=True)

    def product(table_part, values):
        return jnp.einsum("fp,bpr->bfr", table_part, values, preferred_element_type=jnp.float32)

    mixed_real = product(dop_real, columns[0]) - product(dop_imag, columns[1])
    mixed_imag = product(dop_real, columns[1]) + product(dop_imag, columns[0])
    power_part = lax.all_to_all(
        mixed_real * mixed_real + mixed_imag * mixed_imag,
        "pulse",
        split_axis=1,
        concat_axis=2,
        tiled=True,
    )
    halo_width = GUARD + TRAIN
    padded = padded_2(power_part, (("range", 2),), halo_width)
    window_sum = jnp.zeros_like(power_part)
    for offset in range(1, TRAIN + 1):
        left_start = halo_width - GUARD - offset
        right_start = halo_width + GUARD + offset
        window_sum = (
            window_sum
            + padded[:, :, left_start : left_start + gate_count]
            + padded[:, :, right_start : right_start + gate_count]
        )
    noise_level = window_sum / (2.0 * TRAIN)
    return power_part / (noise_level + NOISE_FLOOR)


def solution(mesh):
    chans, pulses_n, halves = (mesh.shape[a] for a in ("chan", "pulse", "range"))

    def step(signal, steering, spectrum):
        split = (
            chans == 4
            and halves == 2
            and steering.shape[1] == chans * pulses_n * halves
            and signal.shape[2] == 2 * pulses_n * (chans // 2) * halves
        )
        if split:
            devices = mesh.devices.reshape(2, chans // 2, pulses_n, halves)
            grid = jax.sharding.Mesh(devices, ("hi", "lo", "pulse", "range"))
            chan, body = ("hi", "lo"), lines
        else:
            grid, chan, body = mesh, "chan", blocks
        return jax.shard_map(
            body,
            mesh=grid,
            in_specs=(P(None, chan, "pulse", "range"), P(), P()),
            out_specs=P(chan, "pulse", "range"),
            check_vma=False,
        )(signal, steering, spectrum)

    return step
```
